256 devices in a mesh: ep: 128 (over x, z, y), dp: 2 (over core).
Axes of the slice: x: 4, y: 4, z: 8, core: 2. Of those that a mesh axis runs over, the one named last changes fastest.
Arguments:
- tokens: bfloat16 [32768, 768], P(('ep', 'dp')), may hold values from -6 to 6
- routing: int32 [32768, 1], P(('ep', 'dp')), may hold values from 0 to 127; in each aligned block of 128 rows (0 to 127, 128 to 255, ...) at most 2 rows name the same one
- gate_prob: float32 [32768], P(('ep', 'dp')), may hold values from 0.2 to 1
- up_weight: bfloat16 [128, 768, 3072], P('ep', None, 'dp'), may hold values from -0.21875 to 0.21875
- down_weight: bfloat16 [128, 3072, 768], P('ep', 'dp'), may hold values from -0.109375 to 0.109375
- out_grad: bfloat16 [32768, 768], P(('ep', 'dp')), may hold values from -1.5 to 1.5
Outputs:
- output: bfloat16 [32768, 768], P(('ep', 'dp'))
- token_grad: bfloat16 [32768, 768], P(('ep', 'dp'))
- prob_grad: float32 [32768], P(('ep', 'dp'))
- up_grad: bfloat16 [128, 768, 3072], P('ep', None, 'dp')
- down_grad: bfloat16 [128, 3072, 768], P('ep', 'dp')
The draws below stay inside these ranges and needn't reach their ends.
Inputs may be any that keep to these rules, and one draw needn't show every extreme that they name: `routing`: among the 128 rows of one device (devices in the order of ep, then dp) no expert is named more than 2 times; in some devices' rows some expert is named exactly 2 times; every expert is named somewhere.
All inputs are finite; a program needn't handle non-finite values.
Results may differ from the reference program's by a relative error of at most 0.0058.
Values may be sent and summed in bfloat16 or wider, within the bound.
No kernel may reach another device: no remote copies, remote signals or barrier semaphores. Data moves between devices by JAX's collectives and lax.ppermute only.
A program may use at most 64 MiB of HBM per device.

```python
import math
import jax
import jax.numpy as jnp
import numpy as np
from jax import lax

D = 768
FF = 3072
TOK_DEV = 128
EXPERTS = 128
CAP = 2
TOKENS = 32768
N_EP = 128
N_DP = 2


def levels(rng, extent, split, least, top_value):
    gain = 1.0
    for position, parts in split:
        heights = jax.random.uniform(jax.random.fold_in(jax.random.fold_in(rng, 6), position), (parts,), jnp.float32, least / len(split), top_value / len(split))
        gain = gain * jnp.repeat(jnp.exp(heights), extent[position] // parts).reshape((-1,) + (1,) * (len(extent) - 1 - position))
    return gain


def shared_out(own_key, own, number, rows, count, top, reach, lean):
    order = jax.random.permutation(own_key, count)
    crowded, ordinary = portions_of(count, rows * top, reach, lean, True), portions_of(count, rows * top, reach, lean, False)
    places = jnp.arange(count)

    def named(sizes, turn):
        used = int((sizes > 0).sum())
        fixed = max(1, used // 4)
        moved = fixed + (places - fixed + turn * (used - fixed)) % max(1, count - fixed)
        return jnp.zeros((count,), jnp.int32).at[order[jnp.where(places < fixed, places, moved)]].set(jnp.asarray(sizes, jnp.int32))

    sizes = jnp.where(number % 4 == 0, named(crowded, number // 4), named(ordinary, number - number // 4 - 1))
    mixed = jax.random.permutation(jax.random.fold_in(own, 3), count)
    source_of, receiver = mixed[0:count // 2 * 2:2], mixed[1:count // 2 * 2:2]
    room = jnp.minimum(sizes[source_of] - 1, reach - sizes[receiver]) // 2
    room = jnp.where((source_of == order[0]) | (receiver == order[0]) | (sizes[receiver] == 0), 0, jnp.maximum(room, 0))
    moved = jax.random.randint(jax.random.fold_in(own, 4), (count // 2,), 0, 1 << 20) % (room + 1)
    sizes = sizes.at[source_of].add(-moved).at[receiver].add(moved)
    members = jnp.searchsorted(jnp.cumsum(sizes), jnp.arange(rows * top), side="right").astype(jnp.int32)
    listing = members.reshape(top, rows).T
    listing = listing[jax.random.permutation(jax.random.fold_in(own, 1), rows)]
    turn = jax.random.randint(jax.random.fold_in(own, 2), (rows, 1), 0, top)
    return jnp.take_along_axis(listing, (jnp.arange(top)[None, :] + turn) % top, axis=1)


def portions_of(number_of, total, limit, slope, full):
    portions = [(1 << 20) // math.isqrt(standing ** slope) + 1 for standing in range(1, number_of + 1)]
    largest = limit if full else min(limit, max(-(-total // number_of), total * portions[0] // sum(portions)))
    least = 1 if total - largest >= number_of - 1 else 0
    holding, rest = [largest] + [least] * (number_of - 1), total - largest - least * (number_of - 1)
    while rest > 0:
        movable = [i for i in range(1, number_of) if holding[i] < largest] or [i for i in range(1, number_of) if holding[i] < limit]
        pool, budget = sum([portions[i] for i in movable]), rest
        for i in movable:
            addition = min(limit - holding[i], max(1, budget * portions[i] // pool), rest)
            holding[i] = holding[i] + addition
            rest = rest - addition
    return np.array(holding)


def normal_values(rng, shape, width, limit, pieces=(), kind=jnp.bfloat16):
    loudness = levels(rng, shape, pieces, -0.22, 0.18) if pieces else 1.0
    entries = jax.random.normal(rng, shape, jnp.float32) * width * loudness
    return jnp.minimum(jnp.maximum(entries, -limit), limit).astype(kind)


def setup_inputs(seed: int = 0) -> dict:
    keys = jax.random.split(jax.random.key(seed), 7)
    tokens = normal_values(keys[0], (TOKENS, D), 1.0, 6.0, ((0, 256),))
    routing_keys = jax.random.split(jax.random.fold_in(keys[1], 1), TOKENS // TOK_DEV)
    routing_turns = jax.random.permutation(jax.random.fold_in(keys[1], 3), TOKENS // TOK_DEV)
    routing = jax.vmap(lambda own, number: shared_out(jax.random.fold_in(keys[1], 2), own, number, TOK_DEV, EXPERTS, 1, CAP, 1))(routing_keys, routing_turns).reshape((TOKENS, 1))
    gate_prob = jnp.clip(0.2 + 0.8 * jax.random.uniform(keys[2], (TOKENS,), jnp.float32) ** levels(keys[2], (TOKENS,), ((0, 256),), -0.2, 0.2), 0.2, 1.0)
    up_weight = normal_values(keys[3], (EXPERTS, D, FF), D ** -0.5, 0.21875, ((0, 128), (2, 2)))
    down_weight = normal_values(keys[4], (EXPERTS, FF, D), FF ** -0.5, 0.109375, ((0, 128), (1, 2)))
    out_grad = normal_values(keys[5], (TOKENS, D), 0.25, 1.5, ((0, 256),))
    return dict(tokens=tokens, routing=routing, gate_prob=gate_prob, up_weight=up_weight, down_weight=down_weight, out_grad=out_grad)


def one_expert(packed):
    rows_in, up_mat, down_mat, grad_in = packed
    up_full = up_mat.astype(jnp.float32)
    down_full = down_mat.astype(jnp.float32)
    preact = jnp.dot(rows_in.astype(jnp.float32), up_full)
    activated, back_fn = jax.vjp(jax.nn.gelu, preact)
    hidden = activated.astype(jnp.bfloat16)
    hidden_wide = hidden.astype(jnp.float32)
    result_rows = jnp.dot(hidden_wide, down_full).astype(jnp.bfloat16)
    grad_wide = grad_in.astype(jnp.float32)
    hidden_grad = jnp.dot(grad_wide, down_full.T)
    preact_grad = back_fn(hidden_grad)[0].astype(jnp.bfloat16)
    preact_wide = preact_grad.astype(jnp.float32)
    input_rows = jnp.dot(preact_wide, up_full.T).astype(jnp.bfloat16)
    up_sum = jnp.dot(rows_in.astype(jnp.float32).T, preact_wide).astype(jnp.bfloat16)
    down_sum = jnp.dot(hidden_wide.T, grad_wide).astype(jnp.bfloat16)
    return (result_rows, input_rows, up_sum, down_sum)

def reference(tokens, routing, gate_prob, up_weight, down_weight, out_grad):
    sources = N_EP * N_DP
    expert = routing[:, 0].astype(jnp.int32)
    onehot = (expert[:, None] == jnp.arange(EXPERTS, dtype=jnp.int32)[None, :]).astype(jnp.int32)
    blocks = onehot.reshape(sources, TOK_DEV, EXPERTS)
    ranking = lax.optimization_barrier(jnp.sum((jnp.cumsum(blocks, axis=1) - blocks) * blocks, axis=2)).reshape(-1)
    source = jnp.arange(TOKENS, dtype=jnp.int32) // TOK_DEV
    column = (source * CAP + ranking).astype(jnp.int32)
    empty = jnp.zeros((EXPERTS, sources * CAP, D), jnp.bfloat16)
    rows_all = empty.at[expert, column].set(tokens)
    scaled = (gate_prob[:, None] * out_grad.astype(jnp.float32)).astype(jnp.bfloat16)
    grads_all = empty.at[expert, column].set(scaled)
    results, inputs, up_grad, down_grad = lax.map(one_expert, (rows_all, up_weight, down_weight, grads_all))
    expert_out = results[expert, column].astype(jnp.float32)
    output = (gate_prob[:, None] * expert_out).astype(jnp.bfloat16)
    prob_grad = lax.optimization_barrier(jnp.sum(out_grad.astype(jnp.float32) * expert_out, axis=1))
    token_grad = inputs[expert, column]
    return (output, token_grad, prob_grad, up_grad, down_grad)
```

```python
import jax
import jax.numpy as jnp
from jax import lax
from jax.sharding import PartitionSpec as P


def local(tokens, routing, gate_prob, up_weight, down_weight, out_grad):
    token_count, width = tokens.shape
    experts = up_weight.shape[0] * lax.axis_size("ep")
    capacity = max(2, 2 * token_count // experts)
    slots = experts * capacity

    def swap(value):
        return lax.ppermute(value, "dp", [(0, 1), (1, 0)])

    up_own, down_own = up_weight[0], down_weight[0]
    up_far, down_far = swap(up_own), swap(down_own)

    expert = routing[:, 0]
    earlier = jnp.arange(token_count)[:, None] > jnp.arange(token_count)[None, :]
    same = (expert[:, None] == expert[None, :]) & earlier
    target = expert * capacity + jnp.sum(same.astype(jnp.int32), axis=1)
    placing = (jnp.arange(slots, dtype=jnp.int32)[:, None] == target[None, :]).astype(jnp.bfloat16)
    grad_wide = out_grad.astype(jnp.float32)
    scaled = (gate_prob[:, None] * grad_wide).astype(jnp.bfloat16)
    both = jnp.concatenate([tokens, scaled], axis=1)
    packed = jnp.dot(placing, both, preferred_element_type=jnp.float32).astype(jnp.bfloat16)

    def exchange(value):
        value = value.reshape(experts, capacity, 2 * width)
        return lax.all_to_all(value, "ep", 0, 0, tiled=True).reshape(slots, 2 * width)

    received = exchange(packed)
    rows, grads = received[:, :width], received[:, width:]
    dot = lambda a, b, dims: lax.dot_general(
        a, b, ((dims[:1], dims[1:]), ((), ())), preferred_element_type=jnp.float32
    )

    def half(up, down):
        preact = dot(rows, up, (1, 0))
        activated, back_fn = jax.vjp(jax.nn.gelu, preact)
        hidden = activated.astype(jnp.bfloat16)
        hidden_grad = dot(grads, down, (1, 1))
        preact_grad = back_fn(hidden_grad)[0].astype(jnp.bfloat16)
        return hidden, preact_grad

    hidden_own, preact_grad_own = half(up_own, down_own)
    hidden_far, preact_grad_far = half(up_far, down_far)
    result = dot(hidden_own, down_own, (1, 0)) + dot(hidden_far, down_far, (1, 0))
    token_side = dot(preact_grad_own, up_own, (1, 1)) + dot(preact_grad_far, up_far, (1, 1))
    sent_back = jnp.concatenate([result, token_side], axis=1).astype(jnp.bfloat16)
    returned = exchange(sent_back)

    received_far = swap(received)
    hidden_near, preact_grad_near = swap(hidden_far), swap(preact_grad_far)
    rows_all = jnp.concatenate([rows, received_far[:, :width]], axis=0)
    grads_all = jnp.concatenate([grads, received_far[:, width:]], axis=0)
    hidden_all = jnp.concatenate([hidden_own, hidden_near], axis=0)
    preact_grad_all = jnp.concatenate([preact_grad_own, preact_grad_near], axis=0)
    up_grad = dot(rows_all, preact_grad_all, (0, 0)).astype(jnp.bfloat16)[None]
    down_grad = dot(hidden_all, grads_all, (0, 0)).astype(jnp.bfloat16)[None]

    collected = dot(placing, returned, (0, 0))
    expert_tok = collected[:, :width]
    output = (gate_prob[:, None] * expert_tok).astype(jnp.bfloat16)
    prob_grad = jnp.sum(grad_wide * expert_tok, axis=1)
    token_grad = collected[:, width:].astype(jnp.bfloat16)
    return (output, token_grad, prob_grad, up_grad, down_grad)


def solution(mesh):
    rows = P(("ep", "dp"), None)
    flat = P(("ep", "dp"))
    up, down = P("ep", None, "dp"), P("ep", "dp", None)
    return jax.shard_map(
        local,
        mesh=mesh,
        in_specs=(rows, rows, flat, up, down, rows),
        out_specs=(rows, rows, flat, up, down),
        check_vma=False,
    )
```

```python
import functools
import math

import jax
import jax.numpy as jnp
from jax import lax
from jax.experimental import pallas as pl
from jax.experimental.pallas import tpu as pltpu
from jax.sharding import PartitionSpec as P

F32 = jnp.float32
BF16 = jnp.bfloat16
GELU_SLOPE = math.sqrt(2.0 / math.pi)
GELU_CUBIC = 0.044715
PIECES = 4
BLOCK = 256


def dot(a, b, dims):
    return lax.dot_general(a, b, ((dims[:1], dims[1:]), ((), ())), preferred_element_type=F32)


def iota(shape, dim):
    return lax.broadcasted_iota(jnp.int32, shape, dim)


def columns(row, n):
    return jnp.transpose(jnp.broadcast_to(row, (n, n)))


def near(value):
    return pltpu.with_memory_space_constraint(value, pltpu.VMEM)


def far(value):
    return pltpu.with_memory_space_constraint(value, pltpu.HBM)


def prep_body(tokens_ref, routing_ref, gate_ref, grad_ref, packed_ref, target_ref):
    n, width = tokens_ref.shape
    piece = width // 2
    expert_row = routing_ref[...]
    same = (columns(expert_row, n) == expert_row) & (iota((n, n), 0) < iota((n, n), 1))
    rank = jnp.sum(same.astype(jnp.int32), axis=0, keepdims=True)
    target = (2 * expert_row + rank) * PIECES
    target_ref[...] = target
    slots = jnp.concatenate([target + k for k in range(PIECES)], axis=1)
    total = packed_ref.shape[0]
    placing = (iota((total, PIECES * n), 0) == slots).astype(F32).astype(BF16)
    gate = columns(gate_ref[...], n)
    gate = jnp.concatenate([gate] * (piece // n), axis=1)
    left = (gate * grad_ref[:, :piece].astype(F32)).astype(BF16)
    right = (gate * grad_ref[:, piece:].astype(F32)).astype(BF16)
    values = jnp.concatenate([tokens_ref[:, :piece], tokens_ref[:, piece:], left, right], axis=0)
    packed_ref[...] = dot(placing, values, (1, 0)).astype(BF16)


def prepare(tokens, routing, gate_prob, out_grad, slots):
    n, width = tokens.shape
    return pl.pallas_call(
        prep_body,
        out_shape=(
            pltpu.VMEM((slots * PIECES, width // 2), BF16),
            pltpu.VMEM((1, n), jnp.int32),
        ),
        compiler_params=pltpu.CompilerParams(vmem_limit_bytes=8 << 20),
        name="prep",
    )(*[far(v) for v in (tokens, routing.reshape(1, n), gate_prob.reshape(1, n), out_grad)])


def reorder_matrix(n, inverse):
    i, j = iota((n, n), 0), iota((n, n), 1)
    if inverse:
        i, j = j, i
    group = n // PIECES
    return (j == (i % group) * PIECES + i // group).astype(F32).astype(BF16)


def mid_body(
    recv_ref, up_hbm, down_hbm, up_far, down_far,
    back_hbm, rows_ref, hidden_hbm, pg_hbm, hidden_far, pg_far,
    up_own, down_own, back, hidden_own, pg_own, result, token_side, weight_sems, act_sems, back_sems,
):
    total, piece = recv_ref.shape
    width = 2 * piece
    chunk = 256
    group = chunk // PIECES

    fetches = (
        pltpu.make_async_copy(up_hbm, up_own, weight_sems.at[0]),
        pltpu.make_async_copy(down_hbm, down_own, weight_sems.at[1]),
    )
    for fetch in fetches:
        fetch.start()

    mix = reorder_matrix(chunk, False)
    for b in range(total // chunk):
        got = dot(mix, recv_ref[b * chunk : (b + 1) * chunk, :], (1, 0)).astype(BF16)
        for k in range(PIECES):
            rows_ref[b * group : (b + 1) * group, k * piece : (k + 1) * piece] = got[
                k * group : (k + 1) * group
            ]
    rows = rows_ref[:, :width]
    grads = rows_ref[:, width:]

    blocks = up_far.shape[1] // BLOCK
    parts = [slice(i * BLOCK, (i + 1) * BLOCK) for i in range(blocks)]
    jobs = [(part, up_far, down_far, hidden_far, pg_far) for part in parts]
    jobs += [(part, up_own, down_own, hidden_own, pg_own) for part in parts]
    stores = []

    def enter(job):
        part, up, down, _, _ = job
        return dot(rows, up[:, part], (1, 0)), dot(grads, down[part, :], (1, 1))

    def leave(k, v, hidden_grad):
        part, up, down, hidden_ref, pg_ref = jobs[k]
        sq = v * v
        t = jnp.tanh(v * (GELU_SLOPE + (GELU_SLOPE * GELU_CUBIC) * sq))
        p = 0.5 + 0.5 * t
        slope = p + v * (0.5 - 0.5 * (t * t)) * (GELU_SLOPE + (3 * GELU_SLOPE * GELU_CUBIC) * sq)
        hidden = (v * p).astype(BF16)
        pg = (hidden_grad * slope).astype(BF16)
        hidden_ref[:, part] = hidden
        pg_ref[:, part] = pg
        to_result = dot(hidden, down[part, :], (1, 0))
        to_token = dot(pg, up[:, part], (1, 1))
        if k == 0:
            result[...] = to_result
            token_side[...] = to_token
        else:
            result[...] += to_result
            token_side[...] += to_token
        if k >= blocks:
            for j, (near_ref, hbm_ref) in enumerate(((hidden_own, hidden_hbm), (pg_own, pg_hbm))):
                store = pltpu.make_async_copy(
                    near_ref.at[:, part], hbm_ref.at[:, part], act_sems.at[2 * (k - blocks) + j]
                )
                store.start()
                stores.append(store)

    pending = enter(jobs[0])
    for k in range(len(jobs)):
        if k + 1 == blocks:
            for fetch in fetches:
                fetch.wait()
        following = enter(jobs[k + 1]) if k + 1 < len(jobs) else None
        leave(k, *pending)
        pending = following

    mix = reorder_matrix(chunk, True)
    for b in range(total // chunk):
        part = slice(b * group, (b + 1) * group)
        stack = jnp.concatenate(
            [
                result[part, :piece],
                result[part, piece:],
                token_side[part, :piece],
                token_side[part, piece:],
            ],
            axis=0,
        ).astype(BF16)
        home = slice(b * chunk, (b + 1) * chunk)
        back[home, :] = dot(mix, stack, (1, 0)).astype(BF16)
        store = pltpu.make_async_copy(back.at[home, :], back_hbm.at[home, :], back_sems.at[b])
        store.start()
        stores.append(store)
    for store in stores:
        store.wait()


def expert_pass(received, up_own, down_own, up_far, down_far):
    total, piece = received.shape
    slots, width = total // PIECES, 2 * piece
    hidden = up_own.shape[1]
    vmem = pl.BlockSpec(memory_space=pltpu.VMEM)
    left = pl.BlockSpec(memory_space=pl.ANY)
    act = pltpu.VMEM((slots, hidden), BF16)
    act_hbm = pltpu.HBM((slots, hidden), BF16)
    blocks = hidden // BLOCK
    return pl.pallas_call(
        mid_body,
        in_specs=[vmem, left, left, vmem, vmem],
        out_specs=[left, vmem, left, left, vmem, vmem],
        out_shape=[
            pltpu.HBM((total, piece), BF16),
            pltpu.VMEM((slots, 2 * width), BF16),
            act_hbm, act_hbm, act, act,
        ],
        scratch_shapes=[
            pltpu.VMEM(up_own.shape, BF16),
            pltpu.VMEM(down_own.shape, BF16),
            pltpu.VMEM((total, piece), BF16),
            act, act,
            pltpu.VMEM((slots, width), F32),
            pltpu.VMEM((slots, width), F32),
            pltpu.SemaphoreType.DMA((2,)),
            pltpu.SemaphoreType.DMA((2 * blocks,)),
            pltpu.SemaphoreType.DMA((total // 256,)),
        ],
        compiler_params=pltpu.CompilerParams(vmem_limit_bytes=30 << 20),
        cost_estimate=pl.CostEstimate(
            flops=16 * slots * width * hidden,
            bytes_accessed=8 * width * hidden + 10 * slots * hidden,
            transcendentals=2 * slots * hidden,
        ),
        name="mid",
    )(near(received), far(up_own), far(down_own), near(up_far), near(down_far))


def collect_body(returned_ref, target_ref, gate_ref, grad_ref, output_ref, token_grad_ref, prob_ref):
    n, width = grad_ref.shape
    piece = width // 2
    total = returned_ref.shape[0]
    target = columns(target_ref[...], n)
    target = jnp.concatenate([target] * (total // n), axis=1)
    lane = iota((n, total), 1)
    picking = jnp.concatenate(
        [(lane == target + k).astype(F32).astype(BF16) for k in range(PIECES)], axis=0
    )
    got = dot(picking, returned_ref[...], (1, 0))
    gate = columns(gate_ref[...], n)
    gate = jnp.concatenate([gate] * (piece // n), axis=1)
    prob = jnp.zeros((n, 1), F32)
    for k in range(2):
        part = slice(k * piece, (k + 1) * piece)
        expert_tok = got[k * n : (k + 1) * n]
        output_ref[:, part] = (gate * expert_tok).astype(BF16)
        prob += jnp.sum(grad_ref[:, part].astype(F32) * expert_tok, axis=1, keepdims=True)
        token_grad_ref[:, part] = got[(2 + k) * n : (3 + k) * n].astype(BF16)
    prob_ref[...] = jnp.transpose(jnp.broadcast_to(prob, (n, n)))[:1]


def collect(returned, target, gate_prob, out_grad):
    n, width = out_grad.shape
    half = jax.ShapeDtypeStruct((n, width), BF16)
    output, token_grad, prob = pl.pallas_call(
        collect_body,
        out_shape=(half, half, jax.ShapeDtypeStruct((1, n), F32)),
        compiler_params=pltpu.CompilerParams(vmem_limit_bytes=8 << 20),
        name="collect",
    )(returned, target, gate_prob.reshape(1, n), out_grad)
    return output, token_grad, prob.reshape(n)


def local(tokens, routing, gate_prob, up_weight, down_weight, out_grad):
    token_count, width = tokens.shape
    experts = up_weight.shape[0] * lax.axis_size("ep")
    slots = 2 * experts

    def swap(value):
        return lax.ppermute(value, "dp", [(0, 1), (1, 0)])

    def exchange(value):
        value = value.reshape(experts, 2 * PIECES, width // 2)
        value = lax.all_to_all(value, "ep", 0, 0, tiled=True)
        return value.reshape(slots * PIECES, width // 2)

    up_own, down_own = up_weight[0], down_weight[0]
    packed, target = prepare(tokens, routing, gate_prob, out_grad, slots)
    up_far, down_far = swap(up_own), swap(down_own)
    received = exchange(packed)
    back, rows, hidden_own, pg_own, hidden_far, pg_far = expert_pass(
        received, up_own, down_own, up_far, down_far
    )
    returned = exchange(back)

    rows_all = jnp.concatenate([rows, swap(rows)], axis=0)
    hidden_all = jnp.concatenate([hidden_own, swap(hidden_far)], axis=0)
    pg_all = jnp.concatenate([pg_own, swap(pg_far)], axis=0)
    up_grad = dot(rows_all[:, :width], pg_all, (0, 0)).astype(BF16)[None]
    down_grad = dot(hidden_all, rows_all[:, width:], (0, 0)).astype(BF16)[None]

    output, token_grad, prob_grad = collect(returned, target, gate_prob, out_grad)
    return (output, token_grad, prob_grad, up_grad, down_grad)


def solution(mesh):
    rows = P(("ep", "dp"), None)
    flat = P(("ep", "dp"))
    up, down = P("ep", None, "dp"), P("ep", "dp", None)
    return jax.shard_map(
        local,
        mesh=mesh,
        in_specs=(rows, rows, flat, up, down, rows),
        out_specs=(rows, rows, flat, up, down),
        check_vma=False,
    )
```

```python
import functools
import math

import jax
import jax.numpy as jnp
from jax import lax
from jax.experimental import pallas as pl
from jax.experimental.pallas import tpu as pltpu
from jax.sharding import PartitionSpec as P

F32 = jnp.float32
BF16 = jnp.bfloat16
GELU_SLOPE = math.sqrt(2.0 / math.pi)
GELU_CUBIC = 0.044715
PIECES = 4
BLOCK = 256


def dot(a, b, dims):
    return lax.dot_general(a, b, ((dims[:1], dims[1:]), ((), ())), preferred_element_type=F32)


def iota(shape, dim):
    return lax.broadcasted_iota(jnp.int32, shape, dim)


def columns(row, n):
    return jnp.transpose(jnp.broadcast_to(row, (n, n)))


def near(value):
    return pltpu.with_memory_space_constraint(value, pltpu.VMEM)


def far(value):
    return pltpu.with_memory_space_constraint(value, pltpu.HBM)


def prep_body(tokens_ref, routing_ref, gate_ref, grad_ref, packed_ref, target_ref):
    n, width = tokens_ref.shape
    piece = width // 2
    expert_row = routing_ref[...]
    same = (columns(expert_row, n) == expert_row) & (iota((n, n), 0) < iota((n, n), 1))
    rank = jnp.sum(same.astype(jnp.int32), axis=0, keepdims=True)
    target = (2 * expert_row + rank) * PIECES
    target_ref[...] = target
    slots = jnp.concatenate([target + k for k in range(PIECES)], axis=1)
    total = packed_ref.shape[0]
    placing = (iota((total, PIECES * n), 0) == slots).astype(F32).astype(BF16)
    gate = columns(gate_ref[...], n)
    gate = jnp.concatenate([gate] * (piece // n), axis=1)
    left = (gate * grad_ref[:, :piece].astype(F32)).astype(BF16)
    right = (gate * grad_ref[:, piece:].astype(F32)).astype(BF16)
    values = jnp.concatenate([tokens_ref[:, :piece], tokens_ref[:, piece:], left, right], axis=0)
    packed_ref[...] = dot(placing, values, (1, 0)).astype(BF16)


def prepare(tokens, routing, gate_prob, out_grad, slots):
    n, width = tokens.shape
    return pl.pallas_call(
        prep_body,
        out_shape=(
            pltpu.VMEM((slots * PIECES, width // 2), BF16),
            pltpu.VMEM((1, n), jnp.int32),
        ),
        compiler_params=pltpu.CompilerParams(vmem_limit_bytes=8 << 20),
        name="prep",
    )(*[far(v) for v in (tokens, routing.reshape(1, n), gate_prob.reshape(1, n), out_grad)])


def reorder_matrix(n, inverse):
    i, j = iota((n, n), 0), iota((n, n), 1)
    if inverse:
        i, j = j, i
    group = n // PIECES
    return (j == (i % group) * PIECES + i // group).astype(F32).astype(BF16)


def reorder(recv_ref, rows_ref, top):
    total, piece = recv_ref.shape
    chunk = 256
    group = chunk // PIECES
    mix = reorder_matrix(chunk, False)
    for b in range(total // chunk):
        got = dot(mix, recv_ref[b * chunk : (b + 1) * chunk, :], (1, 0)).astype(BF16)
        for k in range(PIECES):
            rows_ref[top + b * group : top + (b + 1) * group, k * piece : (k + 1) * piece] = got[
                k * group : (k + 1) * group
            ]


def activate(v, hidden_grad):
    sq = v * v
    t = jnp.tanh(v * (GELU_SLOPE + (GELU_SLOPE * GELU_CUBIC) * sq))
    p = 0.5 + 0.5 * t
    slope = p + v * (0.5 - 0.5 * (t * t)) * (GELU_SLOPE + (3 * GELU_SLOPE * GELU_CUBIC) * sq)
    return (v * p).astype(BF16), (hidden_grad * slope).astype(BF16)


def mid_body(
    recv_ref, up_hbm, down_hbm, up_far, down_far,
    back_hbm, rows_ref, hidden_hbm, pg_hbm,
    up_own, down_own, back, hidden_own, pg_own, result, token_side, weight_sems, act_sems, back_sems,
):
    total, piece = recv_ref.shape
    width = 2 * piece
    chunk = 256
    group = chunk // PIECES

    fetches = (
        pltpu.make_async_copy(up_hbm, up_own, weight_sems.at[0]),
        pltpu.make_async_copy(down_hbm, down_own, weight_sems.at[1]),
    )
    for fetch in fetches:
        fetch.start()

    reorder(recv_ref, rows_ref, 0)
    rows = rows_ref[:, :width]
    grads = rows_ref[:, width:]

    blocks = up_far.shape[1] // BLOCK
    parts = [slice(i * BLOCK, (i + 1) * BLOCK) for i in range(blocks)]
    jobs = [(part, up_far, down_far) for part in parts]
    jobs += [(part, up_own, down_own) for part in parts]
    stores = []

    def enter(job):
        part, up, down = job
        return dot(rows, up[:, part], (1, 0)), dot(grads, down[part, :], (1, 1))

    def leave(k, v, hidden_grad):
        part, up, down = jobs[k]
        hidden, pg = activate(v, hidden_grad)
        to_result = dot(hidden, down[part, :], (1, 0))
        to_token = dot(pg, up[:, part], (1, 1))
        if k == 0:
            result[...] = to_result
            token_side[...] = to_token
        else:
            result[...] += to_result
            token_side[...] += to_token
        if k >= blocks:
            hidden_own[:, part] = hidden
            pg_own[:, part] = pg
            for j, (near_ref, hbm_ref) in enumerate(((hidden_own, hidden_hbm), (pg_own, pg_hbm))):
                store = pltpu.make_async_copy(
                    near_ref.at[:, part], hbm_ref.at[:, part], act_sems.at[2 * (k - blocks) + j]
                )
                store.start()
                stores.append(store)

    pending = enter(jobs[0])
    for k in range(len(jobs)):
        if k + 1 == blocks:
            for fetch in fetches:
                fetch.wait()
        following = enter(jobs[k + 1]) if k + 1 < len(jobs) else None
        leave(k, *pending)
        pending = following

    mix = reorder_matrix(chunk, True)
    for b in range(total // chunk):
        part = slice(b * group, (b + 1) * group)
        stack = jnp.concatenate(
            [
                result[part, :piece],
                result[part, piece:],
                token_side[part, :piece],
                token_side[part, piece:],
            ],
            axis=0,
        ).astype(BF16)
        home = slice(b * chunk, (b + 1) * chunk)
        back[home, :] = dot(mix, stack, (1, 0)).astype(BF16)
        store = pltpu.make_async_copy(back.at[home, :], back_hbm.at[home, :], back_sems.at[b])
        store.start()
        stores.append(store)
    for store in stores:
        store.wait()


def expert_pass(received, up_own, down_own, up_far, down_far):
    total, piece = received.shape
    slots, width = total // PIECES, 2 * piece
    hidden = up_own.shape[1]
    vmem = pl.BlockSpec(memory_space=pltpu.VMEM)
    left = pl.BlockSpec(memory_space=pl.ANY)
    act = pltpu.VMEM((slots, hidden), BF16)
    act_hbm = pltpu.HBM((slots, hidden), BF16)
    blocks = hidden // BLOCK
    return pl.pallas_call(
        mid_body,
        in_specs=[vmem, left, left, vmem, vmem],
        out_specs=[left, vmem, left, left],
        out_shape=[
            pltpu.HBM((total, piece), BF16),
            pltpu.VMEM((slots, 2 * width), BF16),
            act_hbm, act_hbm,
        ],
        scratch_shapes=[
            pltpu.VMEM(up_own.shape, BF16),
            pltpu.VMEM(down_own.shape, BF16),
            pltpu.VMEM((total, piece), BF16),
            act, act,
            pltpu.VMEM((slots, width), F32),
            pltpu.VMEM((slots, width), F32),
            pltpu.SemaphoreType.DMA((2,)),
            pltpu.SemaphoreType.DMA((2 * blocks,)),
            pltpu.SemaphoreType.DMA((total // 256,)),
        ],
        compiler_params=pltpu.CompilerParams(vmem_limit_bytes=30 << 20),
        cost_estimate=pl.CostEstimate(
            flops=16 * slots * width * hidden,
            bytes_accessed=8 * width * hidden + 10 * slots * hidden,
            transcendentals=2 * slots * hidden,
        ),
        name="mid",
    )(near(received), far(up_own), far(down_own), near(up_far), near(down_far))


def weight_body(
    far_ref, near_ref, up_ref, down_ref, hidden_ref, pg_ref, up_grad_ref, down_grad_ref, rows, turned
):
    slots, double = near_ref.shape
    width = double // 2

    @pl.when(pl.program_id(0) == 0)
    def _():
        rows[:slots, :] = near_ref[...]
        reorder(far_ref, rows, slots)
        turned[...] = jnp.transpose(rows[:, :width])

    v = dot(rows[slots:, :width], up_ref[...], (1, 0))
    hidden_grad = dot(rows[slots:, width:], down_ref[...], (1, 1))
    hidden, pg = activate(v, hidden_grad)
    hidden = jnp.concatenate([hidden_ref[...], hidden], axis=0)
    pg = jnp.concatenate([pg_ref[...], pg], axis=0)
    up_grad_ref[...] = dot(turned[...], pg, (1, 0)).astype(BF16)
    down_grad_ref[...] = dot(hidden, rows[:, width:], (0, 0)).astype(BF16)


def weight_gradients(received_far, rows, up, down, hidden, pg):
    total, piece = received_far.shape
    slots, double = rows.shape
    width, units = up.shape
    whole = lambda *shape: pl.BlockSpec(shape, lambda i: (0, 0))
    wide = pl.BlockSpec((width, BLOCK), lambda i: (0, i))
    tall = pl.BlockSpec((BLOCK, width), lambda i: (i, 0))
    act = pl.BlockSpec((slots, BLOCK), lambda i: (0, i))
    return pl.pallas_call(
        weight_body,
        grid=(units // BLOCK,),
        in_specs=[whole(total, piece), whole(slots, double), wide, tall, act, act],
        out_specs=[wide, tall],
        out_shape=[
            jax.ShapeDtypeStruct((width, units), BF16),
            jax.ShapeDtypeStruct((units, width), BF16),
        ],
        scratch_shapes=[pltpu.VMEM((2 * slots, double), BF16), pltpu.VMEM((width, 2 * slots), BF16)],
        compiler_params=pltpu.CompilerParams(
            dimension_semantics=("arbitrary",), vmem_limit_bytes=20 << 20
        ),
        cost_estimate=pl.CostEstimate(
            flops=12 * slots * width * units,
            bytes_accessed=8 * width * units + 8 * slots * double,
            transcendentals=slots * units,
        ),
        name="weights",
    )(received_far, rows, *[far(v) for v in (up, down, hidden, pg)])


def collect_body(returned_ref, target_ref, gate_ref, grad_ref, output_ref, token_grad_ref, prob_ref):
    n, width = grad_ref.shape
    piece = width // 2
    total = returned_ref.shape[0]
    target = columns(target_ref[...], n)
    target = jnp.concatenate([target] * (total // n), axis=1)
    lane = iota((n, total), 1)
    picking = jnp.concatenate(
        [(lane == target + k).astype(F32).astype(BF16) for k in range(PIECES)], axis=0
    )
    got = dot(picking, returned_ref[...], (1, 0))
    gate = columns(gate_ref[...], n)
    gate = jnp.concatenate([gate] * (piece // n), axis=1)
    prob = jnp.zeros((n, 1), F32)
    for k in range(2):
        part = slice(k * piece, (k + 1) * piece)
        expert_tok = got[k * n : (k + 1) * n]
        output_ref[:, part] = (gate * expert_tok).astype(BF16)
        prob += jnp.sum(grad_ref[:, part].astype(F32) * expert_tok, axis=1, keepdims=True)
        token_grad_ref[:, part] = got[(2 + k) * n : (3 + k) * n].astype(BF16)
    prob_ref[...] = jnp.transpose(jnp.broadcast_to(prob, (n, n)))[:1]


def collect(returned, target, gate_prob, out_grad):
    n, width = out_grad.shape
    half = jax.ShapeDtypeStruct((n, width), BF16)
    output, token_grad, prob = pl.pallas_call(
        collect_body,
        out_shape=(half, half, jax.ShapeDtypeStruct((1, n), F32)),
        compiler_params=pltpu.CompilerParams(vmem_limit_bytes=8 << 20),
        name="collect",
    )(returned, target, gate_prob.reshape(1, n), out_grad)
    return output, token_grad, prob.reshape(n)


def local(tokens, routing, gate_prob, up_weight, down_weight, out_grad):
    token_count, width = tokens.shape
    experts = up_weight.shape[0] * lax.axis_size("ep")
    slots = 2 * experts

    def swap(value):
        return lax.ppermute(value, "dp", [(0, 1), (1, 0)])

    def exchange(value):
        value = value.reshape(experts, 2 * PIECES, width // 2)
        value = lax.all_to_all(value, "ep", 0, 0, tiled=True)
        return value.reshape(slots * PIECES, width // 2)

    up_own, down_own = up_weight[0], down_weight[0]
    packed, target = prepare(tokens, routing, gate_prob, out_grad, slots)
    up_far, down_far = swap(up_own), swap(down_own)
    received = exchange(packed)
    received_far = swap(received)
    back, rows, hidden, pg = expert_pass(received, up_own, down_own, up_far, down_far)
    returned = exchange(back)
    up_grad, down_grad = weight_gradients(received_far, rows, up_own, down_own, hidden, pg)
    output, token_grad, prob_grad = collect(returned, target, gate_prob, out_grad)
    return (output, token_grad, prob_grad, up_grad[None], down_grad[None])


def solution(mesh):
    rows = P(("ep", "dp"), None)
    flat = P(("ep", "dp"))
    up, down = P("ep", None, "dp"), P("ep", "dp", None)
    return jax.shard_map(
        local,
        mesh=mesh,
        in_specs=(rows, rows, flat, up, down, rows),
        out_specs=(rows, rows, flat, up, down),
        check_vma=False,
    )
```

```python
import functools
import math

import jax
import jax.numpy as jnp
from jax import lax
from jax.experimental import pallas as pl
from jax.experimental.pallas import tpu as pltpu
from jax.sharding import PartitionSpec as P

F32 = jnp.float32
BF16 = jnp.bfloat16
GELU_SLOPE = math.sqrt(2.0 / math.pi)
GELU_CUBIC = 0.044715
PIECES = 4
EP_X, EP_Z, EP_Y = 4, 8, 4
BLOCK = 256


def place_of(expert, core):
    x, z, y = expert >> 5, (expert >> 2) & (EP_Z - 1), expert & (EP_Y - 1)
    place = (z * EP_X + x) * EP_Y + y
    return place + core * (EP_X * EP_Z * EP_Y - 1 - 2 * place)


def participants():
    walk = [
        (x * EP_Z + z) * EP_Y + y for z in range(EP_Z) for x in range(EP_X) for y in range(EP_Y)
    ]
    return [[2 * e for e in walk], [2 * e + 1 for e in reversed(walk)]]


def dot(a, b, dims):
    return lax.dot_general(a, b, ((dims[:1], dims[1:]), ((), ())), preferred_element_type=F32)


def iota(shape, dim):
    return lax.broadcasted_iota(jnp.int32, shape, dim)


def columns(row, n):
    return jnp.transpose(jnp.broadcast_to(row, (n, n)))


def near(value):
    return pltpu.with_memory_space_constraint(value, pltpu.VMEM)


def far(value):
    return pltpu.with_memory_space_constraint(value, pltpu.HBM)


def prep_body(tokens_ref, routing_ref, gate_ref, grad_ref, packed_ref, target_ref):
    n, width = tokens_ref.shape
    piece = width // 2
    expert_row = routing_ref[...]
    same = (columns(expert_row, n) == expert_row) & (iota((n, n), 0) < iota((n, n), 1))
    rank = jnp.sum(same.astype(jnp.int32), axis=0, keepdims=True)
    target = (2 * place_of(expert_row, lax.axis_index("dp")) + rank) * PIECES
    target_ref[...] = target
    slots = jnp.concatenate([target + k for k in range(PIECES)], axis=1)
    total = packed_ref.shape[0]
    placing = (iota((total, PIECES * n), 0) == slots).astype(F32).astype(BF16)
    gate = columns(gate_ref[...], n)
    gate = jnp.concatenate([gate] * (piece // n), axis=1)
    left = (gate * grad_ref[:, :piece].astype(F32)).astype(BF16)
    right = (gate * grad_ref[:, piece:].astype(F32)).astype(BF16)
    values = jnp.concatenate([tokens_ref[:, :piece], tokens_ref[:, piece:], left, right], axis=0)
    packed_ref[...] = dot(placing, values, (1, 0)).astype(BF16)


def prepare(tokens, routing, gate_prob, out_grad, slots):
    n, width = tokens.shape
    return pl.pallas_call(
        prep_body,
        out_shape=(
            pltpu.VMEM((slots * PIECES, width // 2), BF16),
            pltpu.VMEM((1, n), jnp.int32),
        ),
        compiler_params=pltpu.CompilerParams(vmem_limit_bytes=8 << 20),
        name="prep",
    )(*[far(v) for v in (tokens, routing.reshape(1, n), gate_prob.reshape(1, n), out_grad)])


def reorder_matrix(n, inverse):
    i, j = iota((n, n), 0), iota((n, n), 1)
    if inverse:
        i, j = j, i
    group = n // PIECES
    return (j == (i % group) * PIECES + i // group).astype(F32).astype(BF16)


def reorder(recv_ref, rows_ref, top):
    total, piece = recv_ref.shape
    chunk = 256
    group = chunk // PIECES
    mix = reorder_matrix(chunk, False)
    for b in range(total // chunk):
        got = dot(mix, recv_ref[b * chunk : (b + 1) * chunk, :], (1, 0)).astype(BF16)
        for k in range(PIECES):
            rows_ref[top + b * group : top + (b + 1) * group, k * piece : (k + 1) * piece] = got[
                k * group : (k + 1) * group
            ]


def activate(v, hidden_grad):
    sq = v * v
    t = jnp.tanh(v * (GELU_SLOPE + (GELU_SLOPE * GELU_CUBIC) * sq))
    p = 0.5 + 0.5 * t
    slope = p + v * (0.5 - 0.5 * (t * t)) * (GELU_SLOPE + (3 * GELU_SLOPE * GELU_CUBIC) * sq)
    return (v * p).astype(BF16), (hidden_grad * slope).astype(BF16)


def mid_body(
    recv_ref, up_hbm, down_hbm, up_far, down_far,
    back_hbm, rows_ref, hidden_hbm, pg_hbm,
    up_own, down_own, back, hidden_own, pg_own, result, token_side, weight_sems, act_sems, back_sems,
):
    total, piece = recv_ref.shape
    width = 2 * piece
    chunk = 256
    group = chunk // PIECES

    fetches = (
        pltpu.make_async_copy(up_hbm, up_own, weight_sems.at[0]),
        pltpu.make_async_copy(down_hbm, down_own, weight_sems.at[1]),
    )
    for fetch in fetches:
        fetch.start()

    reorder(recv_ref, rows_ref, 0)
    rows = rows_ref[:, :width]
    grads = rows_ref[:, width:]

    blocks = up_far.shape[1] // BLOCK
    parts = [slice(i * BLOCK, (i + 1) * BLOCK) for i in range(blocks)]
    jobs = [(part, up_far, down_far) for part in parts]
    jobs += [(part, up_own, down_own) for part in parts]
    stores = []

    def enter(job):
        part, up, down = job
        return dot(rows, up[:, part], (1, 0)), dot(grads, down[part, :], (1, 1))

    def leave(k, v, hidden_grad):
        part, up, down = jobs[k]
        hidden, pg = activate(v, hidden_grad)
        to_result = dot(hidden, down[part, :], (1, 0))
        to_token = dot(pg, up[:, part], (1, 1))
        if k == 0:
            result[...] = to_result
            token_side[...] = to_token
        else:
            result[...] += to_result
            token_side[...] += to_token
        if k >= blocks:
            hidden_own[:, part] = hidden
            pg_own[:, part] = pg
            for j, (near_ref, hbm_ref) in enumerate(((hidden_own, hidden_hbm), (pg_own, pg_hbm))):
                store = pltpu.make_async_copy(
                    near_ref.at[:, part], hbm_ref.at[:, part], act_sems.at[2 * (k - blocks) + j]
                )
                store.start()
                stores.append(store)

    pending = enter(jobs[0])
    for k in range(len(jobs)):
        if k + 1 == blocks:
            for fetch in fetches:
                fetch.wait()
        following = enter(jobs[k + 1]) if k + 1 < len(jobs) else None
        leave(k, *pending)
        pending = following

    mix = reorder_matrix(chunk, True)
    for b in range(total // chunk):
        part = slice(b * group, (b + 1) * group)
        stack = jnp.concatenate(
            [
                result[part, :piece],
                result[part, piece:],
                token_side[part, :piece],
                token_side[part, piece:],
            ],
            axis=0,
        ).astype(BF16)
        home = slice(b * chunk, (b + 1) * chunk)
        back[home, :] = dot(mix, stack, (1, 0)).astype(BF16)
        store = pltpu.make_async_copy(back.at[home, :], back_hbm.at[home, :], back_sems.at[b])
        store.start()
        stores.append(store)
    for store in stores:
        store.wait()


def expert_pass(received, up_own, down_own, up_far, down_far):
    total, piece = received.shape
    slots, width = total // PIECES, 2 * piece
    hidden = up_own.shape[1]
    vmem = pl.BlockSpec(memory_space=pltpu.VMEM)
    left = pl.BlockSpec(memory_space=pl.ANY)
    act = pltpu.VMEM((slots, hidden), BF16)
    act_hbm = pltpu.HBM((slots, hidden), BF16)
    blocks = hidden // BLOCK
    return pl.pallas_call(
        mid_body,
        in_specs=[vmem, left, left, vmem, vmem],
        out_specs=[left, vmem, left, left],
        out_shape=[
            pltpu.HBM((total, piece), BF16),
            pltpu.VMEM((slots, 2 * width), BF16),
            act_hbm, act_hbm,
        ],
        scratch_shapes=[
            pltpu.VMEM(up_own.shape, BF16),
            pltpu.VMEM(down_own.shape, BF16),
            pltpu.VMEM((total, piece), BF16),
            act, act,
            pltpu.VMEM((slots, width), F32),
            pltpu.VMEM((slots, width), F32),
            pltpu.SemaphoreType.DMA((2,)),
            pltpu.SemaphoreType.DMA((2 * blocks,)),
            pltpu.SemaphoreType.DMA((total // 256,)),
        ],
        compiler_params=pltpu.CompilerParams(vmem_limit_bytes=30 << 20),
        cost_estimate=pl.CostEstimate(
            flops=16 * slots * width * hidden,
            bytes_accessed=8 * width * hidden + 10 * slots * hidden,
            transcendentals=2 * slots * hidden,
        ),
        name="mid",
    )(near(received), far(up_own), far(down_own), near(up_far), near(down_far))


def weight_body(
    far_ref, near_ref, up_ref, down_ref, hidden_ref, pg_ref, up_grad_ref, down_grad_ref, rows, turned
):
    slots, double = near_ref.shape
    width = double // 2

    @pl.when(pl.program_id(0) == 0)
    def _():
        rows[:slots, :] = near_ref[...]
        reorder(far_ref, rows, slots)
        turned[...] = jnp.transpose(rows[:, :width])

    v = dot(rows[slots:, :width], up_ref[...], (1, 0))
    hidden_grad = dot(rows[slots:, width:], down_ref[...], (1, 1))
    hidden, pg = activate(v, hidden_grad)
    hidden = jnp.concatenate([hidden_ref[...], hidden], axis=0)
    pg = jnp.concatenate([pg_ref[...], pg], axis=0)
    up_grad_ref[...] = dot(turned[...], pg, (1, 0)).astype(BF16)
    down_grad_ref[...] = dot(hidden, rows[:, width:], (0, 0)).astype(BF16)


def weight_gradients(received_far, rows, up, down, hidden, pg):
    total, piece = received_far.shape
    slots, double = rows.shape
    width, units = up.shape
    whole = lambda *shape: pl.BlockSpec(shape, lambda i: (0, 0))
    wide = pl.BlockSpec((width, BLOCK), lambda i: (0, i))
    tall = pl.BlockSpec((BLOCK, width), lambda i: (i, 0))
    act = pl.BlockSpec((slots, BLOCK), lambda i: (0, i))
    return pl.pallas_call(
        weight_body,
        grid=(units // BLOCK,),
        in_specs=[whole(total, piece), whole(slots, double), wide, tall, act, act],
        out_specs=[wide, tall],
        out_shape=[
            jax.ShapeDtypeStruct((width, units), BF16),
            jax.ShapeDtypeStruct((units, width), BF16),
        ],
        scratch_shapes=[pltpu.VMEM((2 * slots, double), BF16), pltpu.VMEM((width, 2 * slots), BF16)],
        compiler_params=pltpu.CompilerParams(
            dimension_semantics=("arbitrary",), vmem_limit_bytes=20 << 20
        ),
        cost_estimate=pl.CostEstimate(
            flops=12 * slots * width * units,
            bytes_accessed=8 * width * units + 8 * slots * double,
            transcendentals=slots * units,
        ),
        name="weights",
    )(received_far, rows, *[far(v) for v in (up, down, hidden, pg)])


def collect_body(returned_ref, target_ref, gate_ref, grad_ref, output_ref, token_grad_ref, prob_ref):
    n, width = grad_ref.shape
    piece = width // 2
    total = returned_ref.shape[0]
    target = columns(target_ref[...], n)
    target = jnp.concatenate([target] * (total // n), axis=1)
    lane = iota((n, total), 1)
    picking = jnp.concatenate(
        [(lane == target + k).astype(F32).astype(BF16) for k in range(PIECES)], axis=0
    )
    got = dot(picking, returned_ref[...], (1, 0))
    gate = columns(gate_ref[...], n)
    gate = jnp.concatenate([gate] * (piece // n), axis=1)
    prob = jnp.zeros((n, 1), F32)
    for k in range(2):
        part = slice(k * piece, (k + 1) * piece)
        expert_tok = got[k * n : (k + 1) * n]
        output_ref[:, part] = (gate * expert_tok).astype(BF16)
        prob += jnp.sum(grad_ref[:, part].astype(F32) * expert_tok, axis=1, keepdims=True)
        token_grad_ref[:, part] = got[(2 + k) * n : (3 + k) * n].astype(BF16)
    prob_ref[...] = jnp.transpose(jnp.broadcast_to(prob, (n, n)))[:1]


def collect(returned, target, gate_prob, out_grad):
    n, width = out_grad.shape
    half = jax.ShapeDtypeStruct((n, width), BF16)
    output, token_grad, prob = pl.pallas_call(
        collect_body,
        out_shape=(half, half, jax.ShapeDtypeStruct((1, n), F32)),
        compiler_params=pltpu.CompilerParams(vmem_limit_bytes=8 << 20),
        name="collect",
    )(returned, target, gate_prob.reshape(1, n), out_grad)
    return output, token_grad, prob.reshape(n)


def local(tokens, routing, gate_prob, up_weight, down_weight, out_grad):
    token_count, width = tokens.shape
    experts = up_weight.shape[0] * lax.axis_size("ep")
    slots = 2 * experts

    def swap(value):
        return lax.ppermute(value, "dp", [(0, 1), (1, 0)])

    def exchange(value):
        value = value.reshape(experts, 2 * PIECES, width // 2)
        value = lax.all_to_all(
            value, ("ep", "dp"), 0, 0, tiled=True, axis_index_groups=participants()
        )
        return value.reshape(slots * PIECES, width // 2)

    up_own, down_own = up_weight[0], down_weight[0]
    packed, target = prepare(tokens, routing, gate_prob, out_grad, slots)
    up_far, down_far = swap(up_own), swap(down_own)
    received = exchange(packed)
    received_far = swap(received)
    back, rows, hidden, pg = expert_pass(received, up_own, down_own, up_far, down_far)
    returned = exchange(back)
    up_grad, down_grad = weight_gradients(received_far, rows, up_own, down_own, hidden, pg)
    output, token_grad, prob_grad = collect(returned, target, gate_prob, out_grad)
    return (output, token_grad, prob_grad, up_grad[None], down_grad[None])


def solution(mesh):
    rows = P(("ep", "dp"), None)
    flat = P(("ep", "dp"))
    up, down = P("ep", None, "dp"), P("ep", "dp", None)
    return jax.shard_map(
        local,
        mesh=mesh,
        in_specs=(rows, rows, flat, up, down, rows),
        out_specs=(rows, rows, flat, up, down),
        check_vma=False,
    )
```

```python
import functools
import math

import jax
import jax.numpy as jnp
from jax import lax
from jax.experimental import pallas as pl
from jax.experimental.pallas import tpu as pltpu
from jax.sharding import PartitionSpec as P

F32 = jnp.float32
BF16 = jnp.bfloat16
GELU_SLOPE = math.sqrt(2.0 / math.pi)
GELU_CUBIC = 0.044715
PIECES = 4
EP_X, EP_Z, EP_Y = 4, 8, 4
BLOCK = 256


def place_of(expert, core):
    x, z, y = expert >> 5, (expert >> 2) & (EP_Z - 1), expert & (EP_Y - 1)
    place = (z * EP_Y + y) * EP_X + x
    return place + core * (EP_X * EP_Z * EP_Y - 1 - 2 * place)


def participants():
    walk = [
        (x * EP_Z + z) * EP_Y + y for z in range(EP_Z) for y in range(EP_Y) for x in range(EP_X)
    ]
    return [[2 * e for e in walk], [2 * e + 1 for e in reversed(walk)]]


def dot(a, b, dims):
    return lax.dot_general(a, b, ((dims[:1], dims[1:]), ((), ())), preferred_element_type=F32)


def iota(shape, dim):
    return lax.broadcasted_iota(jnp.int32, shape, dim)


def columns(row, n):
    return jnp.transpose(jnp.broadcast_to(row, (n, n)))


def near(value):
    return pltpu.with_memory_space_constraint(value, pltpu.VMEM)


def far(value):
    return pltpu.with_memory_space_constraint(value, pltpu.HBM)


def prep_body(tokens_ref, routing_ref, gate_ref, grad_ref, packed_ref, target_ref):
    n, width = tokens_ref.shape
    piece = width // 2
    expert_row = routing_ref[...]
    same = (columns(expert_row, n) == expert_row) & (iota((n, n), 0) < iota((n, n), 1))
    rank = jnp.sum(same.astype(jnp.int32), axis=0, keepdims=True)
    target = (2 * place_of(expert_row, lax.axis_index("dp")) + rank) * PIECES
    target_ref[...] = target
    slots = jnp.concatenate([target + k for k in range(PIECES)], axis=1)
    total = packed_ref.shape[0]
    placing = (iota((total, PIECES * n), 0) == slots).astype(F32).astype(BF16)
    gate = columns(gate_ref[...], n)
    gate = jnp.concatenate([gate] * (piece // n), axis=1)
    left = (gate * grad_ref[:, :piece].astype(F32)).astype(BF16)
    right = (gate * grad_ref[:, piece:].astype(F32)).astype(BF16)
    values = jnp.concatenate([tokens_ref[:, :piece], tokens_ref[:, piece:], left, right], axis=0)
    packed_ref[...] = dot(placing, values, (1, 0)).astype(BF16)


def prepare(tokens, routing, gate_prob, out_grad, slots):
    n, width = tokens.shape
    return pl.pallas_call(
        prep_body,
        out_shape=(
            pltpu.VMEM((slots * PIECES, width // 2), BF16),
            pltpu.VMEM((1, n), jnp.int32),
        ),
        compiler_params=pltpu.CompilerParams(vmem_limit_bytes=8 << 20),
        name="prep",
    )(*[far(v) for v in (tokens, routing.reshape(1, n), gate_prob.reshape(1, n), out_grad)])


def reorder_matrix(n, inverse):
    i, j = iota((n, n), 0), iota((n, n), 1)
    if inverse:
        i, j = j, i
    group = n // PIECES
    return (j == (i % group) * PIECES + i // group).astype(F32).astype(BF16)


def reorder(recv_ref, rows_ref, top):
    total, piece = recv_ref.shape
    chunk = 256
    group = chunk // PIECES
    mix = reorder_matrix(chunk, False)
    for b in range(total // chunk):
        got = dot(mix, recv_ref[b * chunk : (b + 1) * chunk, :], (1, 0)).astype(BF16)
        for k in range(PIECES):
            rows_ref[top + b * group : top + (b + 1) * group, k * piece : (k + 1) * piece] = got[
                k * group : (k + 1) * group
            ]


def activate(v, hidden_grad):
    sq = v * v
    t = jnp.tanh(v * (GELU_SLOPE + (GELU_SLOPE * GELU_CUBIC) * sq))
    p = 0.5 + 0.5 * t
    slope = p + v * (0.5 - 0.5 * (t * t)) * (GELU_SLOPE + (3 * GELU_SLOPE * GELU_CUBIC) * sq)
    return (v * p).astype(BF16), (hidden_grad * slope).astype(BF16)


def mid_body(
    recv_ref, up_hbm, down_hbm, up_far, down_far,
    back_hbm, rows_ref, hidden_hbm, pg_hbm,
    up_own, down_own, back, hidden_own, pg_own, result, token_side, weight_sems, act_sems, back_sems,
):
    total, piece = recv_ref.shape
    width = 2 * piece
    chunk = 256
    group = chunk // PIECES

    fetches = (
        pltpu.make_async_copy(up_hbm, up_own, weight_sems.at[0]),
        pltpu.make_async_copy(down_hbm, down_own, weight_sems.at[1]),
    )
    for fetch in fetches:
        fetch.start()

    reorder(recv_ref, rows_ref, 0)
    rows = rows_ref[:, :width]
    grads = rows_ref[:, width:]

    blocks = up_far.shape[1] // BLOCK
    parts = [slice(i * BLOCK, (i + 1) * BLOCK) for i in range(blocks)]
    jobs = [(part, up_far, down_far) for part in parts]
    jobs += [(part, up_own, down_own) for part in parts]
    stores = []

    def enter(job):
        part, up, down = job
        return dot(rows, up[:, part], (1, 0)), dot(grads, down[part, :], (1, 1))

    def leave(k, v, hidden_grad):
        part, up, down = jobs[k]
        hidden, pg = activate(v, hidden_grad)
        to_result = dot(hidden, down[part, :], (1, 0))
        to_token = dot(pg, up[:, part], (1, 1))
        if k == 0:
            result[...] = to_result
            token_side[...] = to_token
        else:
            result[...] += to_result
            token_side[...] += to_token
        if k >= blocks:
            hidden_own[:, part] = hidden
            pg_own[:, part] = pg
            for j, (near_ref, hbm_ref) in enumerate(((hidden_own, hidden_hbm), (pg_own, pg_hbm))):
                store = pltpu.make_async_copy(
                    near_ref.at[:, part], hbm_ref.at[:, part], act_sems.at[2 * (k - blocks) + j]
                )
                store.start()
                stores.append(store)

    pending = enter(jobs[0])
    for k in range(len(jobs)):
        if k + 1 == blocks:
            for fetch in fetches:
                fetch.wait()
        following = enter(jobs[k + 1]) if k + 1 < len(jobs) else None
        leave(k, *pending)
        pending = following

    mix = reorder_matrix(chunk, True)
    for b in range(total // chunk):
        part = slice(b * group, (b + 1) * group)
        stack = jnp.concatenate(
            [
                result[part, :piece],
                result[part, piece:],
                token_side[part, :piece],
                token_side[part, piece:],
            ],
            axis=0,
        ).astype(BF16)
        home = slice(b * chunk, (b + 1) * chunk)
        back[home, :] = dot(mix, stack, (1, 0)).astype(BF16)
        store = pltpu.make_async_copy(back.at[home, :], back_hbm.at[home, :], back_sems.at[b])
        store.start()
        stores.append(store)
    for store in stores:
        store.wait()


def expert_pass(received, up_own, down_own, up_far, down_far):
    total, piece = received.shape
    slots, width = total // PIECES, 2 * piece
    hidden = up_own.shape[1]
    vmem = pl.BlockSpec(memory_space=pltpu.VMEM)
    left = pl.BlockSpec(memory_space=pl.ANY)
    act = pltpu.VMEM((slots, hidden), BF16)
    act_hbm = pltpu.HBM((slots, hidden), BF16)
    blocks = hidden // BLOCK
    return pl.pallas_call(
        mid_body,
        in_specs=[vmem, left, left, vmem, vmem],
        out_specs=[left, vmem, left, left],
        out_shape=[
            pltpu.HBM((total, piece), BF16),
            pltpu.VMEM((slots, 2 * width), BF16),
            act_hbm, act_hbm,
        ],
        scratch_shapes=[
            pltpu.VMEM(up_own.shape, BF16),
            pltpu.VMEM(down_own.shape, BF16),
            pltpu.VMEM((total, piece), BF16),
            act, act,
            pltpu.VMEM((slots, width), F32),
            pltpu.VMEM((slots, width), F32),
            pltpu.SemaphoreType.DMA((2,)),
            pltpu.SemaphoreType.DMA((2 * blocks,)),
            pltpu.SemaphoreType.DMA((total // 256,)),
        ],
        compiler_params=pltpu.CompilerParams(vmem_limit_bytes=30 << 20),
        cost_estimate=pl.CostEstimate(
            flops=16 * slots * width * hidden,
            bytes_accessed=8 * width * hidden + 10 * slots * hidden,
            transcendentals=2 * slots * hidden,
        ),
        name="mid",
    )(near(received), far(up_own), far(down_own), near(up_far), near(down_far))


def weight_body(
    far_ref, near_ref, up_ref, down_ref, hidden_ref, pg_ref, up_grad_ref, down_grad_ref, rows, turned
):
    slots, double = near_ref.shape
    width = double // 2

    @pl.when(pl.program_id(0) == 0)
    def _():
        rows[:slots, :] = near_ref[...]
        reorder(far_ref, rows, slots)
        turned[...] = jnp.transpose(rows[:, :width])

    v = dot(rows[slots:, :width], up_ref[...], (1, 0))
    hidden_grad = dot(rows[slots:, width:], down_ref[...], (1, 1))
    hidden, pg = activate(v, hidden_grad)
    hidden = jnp.concatenate([hidden_ref[...], hidden], axis=0)
    pg = jnp.concatenate([pg_ref[...], pg], axis=0)
    up_grad_ref[...] = dot(turned[...], pg, (1, 0)).astype(BF16)
    down_grad_ref[...] = dot(hidden, rows[:, width:], (0, 0)).astype(BF16)


def weight_gradients(received_far, rows, up, down, hidden, pg):
    total, piece = received_far.shape
    slots, double = rows.shape
    width, units = up.shape
    whole = lambda *shape: pl.BlockSpec(shape, lambda i: (0, 0))
    wide = pl.BlockSpec((width, BLOCK), lambda i: (0, i))
    tall = pl.BlockSpec((BLOCK, width), lambda i: (i, 0))
    act = pl.BlockSpec((slots, BLOCK), lambda i: (0, i))
    return pl.pallas_call(
        weight_body,
        grid=(units // BLOCK,),
        in_specs=[whole(total, piece), whole(slots, double), wide, tall, act, act],
        out_specs=[wide, tall],
        out_shape=[
            jax.ShapeDtypeStruct((width, units), BF16),
            jax.ShapeDtypeStruct((units, width), BF16),
        ],
        scratch_shapes=[pltpu.VMEM((2 * slots, double), BF16), pltpu.VMEM((width, 2 * slots), BF16)],
        compiler_params=pltpu.CompilerParams(
            dimension_semantics=("arbitrary",), vmem_limit_bytes=20 << 20
        ),
        cost_estimate=pl.CostEstimate(
            flops=12 * slots * width * units,
            bytes_accessed=8 * width * units + 8 * slots * double,
            transcendentals=slots * units,
        ),
        name="weights",
    )(received_far, rows, *[far(v) for v in (up, down, hidden, pg)])


def collect_body(returned_ref, target_ref, gate_ref, grad_ref, output_ref, token_grad_ref, prob_ref):
    n, width = grad_ref.shape
    piece = width // 2
    total = returned_ref.shape[0]
    target = columns(target_ref[...], n)
    target = jnp.concatenate([target] * (total // n), axis=1)
    lane = iota((n, total), 1)
    picking = jnp.concatenate(
        [(lane == target + k).astype(F32).astype(BF16) for k in range(PIECES)], axis=0
    )
    got = dot(picking, returned_ref[...], (1, 0))
    gate = columns(gate_ref[...], n)
    gate = jnp.concatenate([gate] * (piece // n), axis=1)
    prob = jnp.zeros((n, 1), F32)
    for k in range(2):
        part = slice(k * piece, (k + 1) * piece)
        expert_tok = got[k * n : (k + 1) * n]
        output_ref[:, part] = (gate * expert_tok).astype(BF16)
        prob += jnp.sum(grad_ref[:, part].astype(F32) * expert_tok, axis=1, keepdims=True)
        token_grad_ref[:, part] = got[(2 + k) * n : (3 + k) * n].astype(BF16)
    prob_ref[...] = jnp.transpose(jnp.broadcast_to(prob, (n, n)))[:1]


def collect(returned, target, gate_prob, out_grad):
    n, width = out_grad.shape
    half = jax.ShapeDtypeStruct((n, width), BF16)
    output, token_grad, prob = pl.pallas_call(
        collect_body,
        out_shape=(half, half, jax.ShapeDtypeStruct((1, n), F32)),
        compiler_params=pltpu.CompilerParams(vmem_limit_bytes=8 << 20),
        name="collect",
    )(returned, target, gate_prob.reshape(1, n), out_grad)
    return output, token_grad, prob.reshape(n)


def local(tokens, routing, gate_prob, up_weight, down_weight, out_grad):
    token_count, width = tokens.shape
    experts = up_weight.shape[0] * lax.axis_size("ep")
    slots = 2 * experts

    def swap(value):
        return lax.ppermute(value, "dp", [(0, 1), (1, 0)])

    def exchange(value):
        value = value.reshape(experts, 2 * PIECES, width // 2)
        value = lax.all_to_all(
            value, ("ep", "dp"), 0, 0, tiled=True, axis_index_groups=participants()
        )
        return value.reshape(slots * PIECES, width // 2)

    up_own, down_own = up_weight[0], down_weight[0]
    packed, target = prepare(tokens, routing, gate_prob, out_grad, slots)
    up_far, down_far = swap(up_own), swap(down_own)
    received = exchange(packed)
    received_far = swap(received)
    back, rows, hidden, pg = expert_pass(received, up_own, down_own, up_far, down_far)
    returned = exchange(back)
    up_grad, down_grad = weight_gradients(received_far, rows, up_own, down_own, hidden, pg)
    output, token_grad, prob_grad = collect(returned, target, gate_prob, out_grad)
    return (output, token_grad, prob_grad, up_grad[None], down_grad[None])


def solution(mesh):
    rows = P(("ep", "dp"), None)
    flat = P(("ep", "dp"))
    up, down = P("ep", None, "dp"), P("ep", "dp", None)
    return jax.shard_map(
        local,
        mesh=mesh,
        in_specs=(rows, rows, flat, up, down, rows),
        out_specs=(rows, rows, flat, up, down),
        check_vma=False,
    )
```
